32 devices in a mesh: rep: 16 (over z, y, x), shard: 2 (over core).
Axes of the slice: x: 2, y: 2, z: 4, core: 2. Of those that a mesh axis runs over, the one named last changes fastest.
Arguments:
- params: float32 [16, 1600, 3200], P('rep', None, 'shard'), may hold values from -6 to 6
- momentum: float32 [16, 1600, 3200], P('rep', None, 'shard'), may hold values from -6 to 6
- tokens: bfloat16 [16, 2, 256, 1600], P('rep', None, 'shard'), may hold values from -6 to 6
- targets: bfloat16 [16, 2, 256, 3200], P('rep', None, None, 'shard'), may hold values from -6 to 6
- blend_weight: float32 [3200], P('shard'), may hold values from 0.2 to 0.9
Outputs:
- averaged: float32 [1600, 3200], P(None, 'shard')
- blended: float32 [16, 1600, 3200], P('rep', None, 'shard')
The draws below stay inside these ranges and needn't reach their ends.
All inputs are finite; a program needn't handle non-finite values.
Results may differ from the reference program's by a relative error of at most 0.0045.
Values may be sent and summed in bfloat16 or wider, within the bound.
A program may use at most 128 MiB of HBM per device.

```python
import math
import jax
import jax.numpy as jnp
from jax import lax

D = 1600
FFW = 3200
H = 2
TOKS = 256
REPS = 16


def levels(stream_key, extent, cuts, low, largest):
    def one(position, blocks):
        steps = jax.random.uniform(jax.random.fold_in(jax.random.fold_in(stream_key, 6), position), (blocks,), jnp.float32, low / len(cuts), largest / len(cuts))
        return jnp.repeat(jnp.exp(steps), extent[position] // blocks).reshape((-1,) + (1,) * (len(extent) - position - 1))

    gain = one(*cuts[0])
    for cut in cuts[1:]:
        gain = gain * one(*cut)
    return gain


def scatter_about(stream_key, shape, width, reach, shards=(), dtype=jnp.bfloat16):
    values = width * jax.random.normal(stream_key, shape, jnp.float32)
    if shards:
        values = values * levels(stream_key, shape, shards, -0.22, 0.18)
    return jnp.clip(values, -reach, reach).astype(dtype)


def setup_inputs(seed: int = 0) -> dict:
    arg_keys = jax.random.split(jax.random.key(seed), 6)
    params = scatter_about(arg_keys[0], (REPS, D, FFW), 1.0, 6.0, ((0, 16), (2, 2)), jnp.float32)
    momentum = scatter_about(arg_keys[1], (REPS, D, FFW), 1.0, 6.0, ((0, 16), (2, 2)), jnp.float32)
    tokens = scatter_about(arg_keys[2], (REPS, H, TOKS, D), 1.0, 6.0, ((0, 16), (2, 2)))
    targets = scatter_about(arg_keys[3], (REPS, H, TOKS, FFW), 1.0, 6.0, ((0, 16), (3, 2)))
    blend_weight = jnp.clip(jnp.exp(math.log(0.9) - 1.50407736 * jax.random.uniform(arg_keys[4], (FFW,), jnp.float32) ** levels(arg_keys[4], (FFW,), ((0, 2),), -0.2, 0.2)), 0.2, 0.9)
    return {"params": params, "momentum": momentum, "tokens": tokens, "targets": targets, "blend_weight": blend_weight}


learn_rate = 0.05
momentum_decay = 0.9

def gelu_tanh(value):
    return jax.nn.gelu(value, approximate=True)

def replica(weight, moment, inputs, wanted):
    scaling = 1.0 / jnp.sqrt(jnp.float32(D))
    for local_step in range(H):
        weight_half = weight.astype(jnp.bfloat16)
        pre = jnp.dot(inputs[local_step], weight_half, preferred_element_type=jnp.float32) * scaling
        activation, pullback = jax.vjp(gelu_tanh, pre)
        slope, = pullback(activation - wanted[local_step].astype(jnp.float32))
        hidden_grad = (slope * scaling).astype(jnp.bfloat16)
        gradient = lax.dot_general(inputs[local_step], hidden_grad, (((0,), (0,)), ((), ())), preferred_element_type=jnp.float32)
        moment = momentum_decay * moment + gradient
        weight = weight - learn_rate * moment
    return (weight, moment)

def reference(params, momentum, tokens, targets, blend_weight):
    weights, moments = lax.map(lambda packed: replica(*packed), (params, momentum, tokens, targets))
    averaged = lax.optimization_barrier(jnp.sum(weights, axis=0)) / jnp.float32(REPS)
    mean_moment = lax.optimization_barrier(jnp.sum(moments, axis=0)) / jnp.float32(REPS)
    blended = blend_weight * mean_moment[None] + (1.0 - blend_weight) * moments
    return (averaged, blended)
```

```python
import functools

import jax
import jax.numpy as jnp
from jax import lax
from jax.experimental import pallas as pl
from jax.experimental.pallas import tpu as pltpu
from jax.sharding import PartitionSpec as P

learn_rate = 0.05
momentum_decay = 0.9
ROWS = 8


def gelu_tanh(value):
    return jax.nn.gelu(value, approximate=True)


def bit_order(chunk, bits):
    lead = chunk % 3
    wave = chunk // 3
    rest = list(range(bits))
    if lead == 0 or bits < 3:
        return rest
    if lead == 1:
        return [1, 0] + rest[2:]
    return [2] + ([0, 1] if wave % 2 == 0 else [1, 0]) + rest[3:]


def pieces(first, count, split, total):
    out = []
    for which, (low, high) in enumerate(((0, split), (split, total))):
        begin, end = max(first, low), min(first + count, high)
        if begin < end:
            out.append((which, begin - low, begin - first, end - begin))
    return out


def mean_kernel(n, bits, chunks, weight_hbm, moment_hbm, out_w_hbm, out_m_hbm,
                held, staged, landed, result, load_sem, send_sem, recv_sem, store_sem):
    me = lax.axis_index("rep")
    sources, sinks = (weight_hbm, moment_hbm), (out_w_hbm, out_m_hbm)
    split = weight_hbm.shape[0]
    total = 2 * split

    def side(bit):
        return (me // (1 << bit)) % 2

    def partner(bit):
        return me + (1 - 2 * side(bit)) * (1 << bit)

    loads = []
    for chunk in range(chunks):
        mine = []
        for which, at, offset, count in pieces(chunk * n, n, split, total):
            mine.append(pltpu.make_async_copy(
                sources[which].at[pl.ds(at, count)],
                held.at[pl.ds(chunk * n + offset, count)],
                load_sem.at[chunk, which],
            ))
        for copy in mine:
            copy.start()
        loads.append(mine)
    padding = chunks * n - total
    if padding:
        held[pl.ds(total, padding)] = jnp.zeros((padding,) + held.shape[1:], held.dtype)

    barrier = pltpu.get_barrier_semaphore()
    for bit in range(bits):
        pl.semaphore_signal(barrier, inc=1, device_id={"rep": partner(bit)},
                            device_id_type=pl.DeviceIdType.MESH)
    pl.semaphore_wait(barrier, bits)

    copies = {}
    low = {chunk: [chunk * n] for chunk in range(chunks)}

    def act(chunk, stage):
        order = bit_order(chunk, bits)
        if stage == 0:
            for copy in loads[chunk]:
                copy.wait()
        else:
            copies[chunk, stage - 1].wait_recv()
        if stage < bits:
            bit = order[stage]
            half = n >> (stage + 1)
            start = low[chunk][stage]
            keep = start + side(bit) * half
            give = start + (1 - side(bit)) * half
            slot = chunk * n + (n - 2 * half)
            before = slot - 2 * half

            def step(i, carry):
                if stage == 0:
                    staged[slot + i] = held[give + i].astype(jnp.bfloat16)
                else:
                    staged[slot + i] = (
                        held[give + i]
                        + landed[before + (give - start) + i].astype(jnp.float32)
                    ).astype(jnp.bfloat16)
                return carry

            def keep_step(i, carry):
                held[keep + i] = held[keep + i] + landed[before + (keep - start) + i].astype(jnp.float32)
                return carry

            lax.fori_loop(0, half, step, 0)
            copy = pltpu.make_async_remote_copy(
                src_ref=staged.at[pl.ds(slot, half)],
                dst_ref=landed.at[pl.ds(slot, half)],
                send_sem=send_sem.at[chunk, stage],
                recv_sem=recv_sem.at[chunk, stage],
                device_id={"rep": partner(bit)},
                device_id_type=pl.DeviceIdType.MESH,
            )
            copy.start()
            copies[chunk, stage] = copy
            if stage > 0:
                lax.fori_loop(0, half, keep_step, 0)
            low[chunk].append(keep)
        elif stage < 2 * bits:
            back = 2 * bits - 1 - stage
            bit = order[back]
            size = n >> (back + 1)
            start = low[chunk][back + 1]
            if stage == bits:
                slot = chunk * n + n - 2
                result[start] = (
                    (held[start] + landed[slot].astype(jnp.float32)) * (1.0 / n)
                ).astype(jnp.bfloat16)
            copy = pltpu.make_async_remote_copy(
                src_ref=result.at[pl.ds(start, size)],
                dst_ref=result.at[pl.ds(start, size)],
                send_sem=send_sem.at[chunk, stage],
                recv_sem=recv_sem.at[chunk, stage],
                device_id={"rep": partner(bit)},
                device_id_type=pl.DeviceIdType.MESH,
            )
            copy.start()
            copies[chunk, stage] = copy
        else:
            for which, at, offset, count in pieces(chunk * n, n, split, total):
                copy = pltpu.make_async_copy(
                    result.at[pl.ds(chunk * n + offset, count)],
                    sinks[which].at[pl.ds(at, count)],
                    store_sem.at[chunk, which],
                )
                copy.start()
                stores.append(copy)

    stores = []
    waves = -(-chunks // 3)
    for tick in range(waves + 2 * bits):
        for stage in range(2 * bits, -1, -1):
            wave = tick - stage
            if 0 <= wave < waves:
                for chunk in range(3 * wave, min(3 * wave + 3, chunks)):
                    act(chunk, stage)
    for copy in copies.values():
        copy.wait_send()
    for copy in stores:
        copy.wait()


def replica_means(weight, moment):
    n = lax.axis_size("rep")
    bits = n.bit_length() - 1
    assert n == 1 << bits
    rows, columns = weight.shape
    slabs = rows // ROWS
    chunks = -(-2 * slabs // n)
    space = chunks * n
    shape = (slabs, ROWS, columns)
    out = jax.ShapeDtypeStruct(shape, jnp.bfloat16)
    sent = chunks * 2 * (n - 1) * ROWS * columns * 2
    means = pl.pallas_call(
        functools.partial(mean_kernel, n, bits, chunks),
        out_shape=(out, out),
        in_specs=[pl.BlockSpec(memory_space=pl.ANY)] * 2,
        out_specs=(pl.BlockSpec(memory_space=pl.ANY),) * 2,
        scratch_shapes=[
            pltpu.VMEM((space, ROWS, columns), jnp.float32),
            pltpu.VMEM((space, ROWS, columns), jnp.bfloat16),
            pltpu.VMEM((space, ROWS, columns), jnp.bfloat16),
            pltpu.VMEM((space, ROWS, columns), jnp.bfloat16),
            pltpu.SemaphoreType.DMA((chunks, 2)),
            pltpu.SemaphoreType.DMA((chunks, 2 * bits)),
            pltpu.SemaphoreType.DMA((chunks, 2 * bits)),
            pltpu.SemaphoreType.DMA((chunks, 2)),
        ],
        compiler_params=pltpu.CompilerParams(
            collective_id=0, has_side_effects=True, vmem_limit_bytes=62 * 1024 * 1024
        ),
        cost_estimate=pl.CostEstimate(flops=0, bytes_accessed=sent, transcendentals=0),
    )(weight.reshape(shape), moment.reshape(shape))
    return tuple(mean.reshape(rows, columns).astype(jnp.float32) for mean in means)


def local(params, momentum, tokens, targets, blend_weight):
    inputs = lax.all_gather(tokens[0], "shard", axis=1, tiled=True)
    wanted = targets[0]
    weight = params[0]
    moment = momentum[0]
    scaling = 1.0 / jnp.sqrt(jnp.float32(weight.shape[0]))
    for local_step in range(inputs.shape[0]):
        weight_half = weight.astype(jnp.bfloat16)
        pre = jnp.dot(inputs[local_step], weight_half, preferred_element_type=jnp.float32) * scaling
        activation, pullback = jax.vjp(gelu_tanh, pre)
        (slope,) = pullback(activation - wanted[local_step].astype(jnp.float32))
        hidden_grad = (slope * scaling).astype(jnp.bfloat16)
        gradient = lax.dot_general(
            inputs[local_step],
            hidden_grad,
            (((0,), (0,)), ((), ())),
            preferred_element_type=jnp.float32,
        )
        moment = momentum_decay * moment + gradient
        weight = weight - learn_rate * moment
    averaged, mean_moment = replica_means(weight, moment)
    blended = blend_weight * mean_moment + (1.0 - blend_weight) * moment
    return (averaged, blended[None])


def solution(mesh):
    return jax.shard_map(
        local,
        mesh=mesh,
        in_specs=(
            P("rep", None, "shard"),
            P("rep", None, "shard"),
            P("rep", None, "shard", None),
            P("rep", None, None, "shard"),
            P("shard"),
        ),
        out_specs=(P(None, "shard"), P("rep", None, "shard")),
        check_vma=False,
    )
```

```python
import functools

import jax
import jax.numpy as jnp
from jax import lax
from jax.experimental import pallas as pl
from jax.experimental.pallas import tpu as pltpu
from jax.sharding import PartitionSpec as P

learn_rate = 0.05
momentum_decay = 0.9
ROWS = 8


def bit_order(chunk, bits):
    lead = chunk % 3
    wave = chunk // 3
    rest = list(range(bits))
    if lead == 0 or bits < 3:
        return rest
    if lead == 1:
        return [1, 0] + rest[2:]
    return [2] + ([0, 1] if wave % 2 == 0 else [1, 0]) + rest[3:]


def pieces(first, count, split, total):
    out = []
    for which, (low, high) in enumerate(((0, split), (split, total))):
        begin, end = max(first, low), min(first + count, high)
        if begin < end:
            out.append((which, begin - low, begin - first, end - begin))
    return out


def mean_kernel(n, bits, chunks, weight_hbm, moment_hbm, out_w_hbm, out_m_hbm,
                held, staged, landed, result, load_sem, send_sem, recv_sem, store_sem):
    me = lax.axis_index("rep")
    sources, sinks = (weight_hbm, moment_hbm), (out_w_hbm, out_m_hbm)
    split = weight_hbm.shape[0]
    total = 2 * split

    def side(bit):
        return (me // (1 << bit)) % 2

    def partner(bit):
        return me + (1 - 2 * side(bit)) * (1 << bit)

    loads = []
    for chunk in range(chunks):
        mine = []
        for which, at, offset, count in pieces(chunk * n, n, split, total):
            mine.append(pltpu.make_async_copy(
                sources[which].at[pl.ds(at, count)],
                held.at[pl.ds(chunk * n + offset, count)],
                load_sem.at[chunk, which],
            ))
        for copy in mine:
            copy.start()
        loads.append(mine)
    padding = chunks * n - total
    if padding:
        held[pl.ds(total, padding)] = jnp.zeros((padding,) + held.shape[1:], held.dtype)

    barrier = pltpu.get_barrier_semaphore()
    for bit in range(bits):
        pl.semaphore_signal(barrier, inc=1, device_id={"rep": partner(bit)},
                            device_id_type=pl.DeviceIdType.MESH)
    pl.semaphore_wait(barrier, bits)

    copies = {}
    low = {chunk: [chunk * n] for chunk in range(chunks)}

    def act(chunk, stage):
        order = bit_order(chunk, bits)
        if stage == 0:
            for copy in loads[chunk]:
                copy.wait()
        else:
            copies[chunk, stage - 1].wait_recv()
        if stage < bits:
            bit = order[stage]
            half = n >> (stage + 1)
            start = low[chunk][stage]
            keep = start + side(bit) * half
            give = start + (1 - side(bit)) * half
            slot = chunk * n + (n - 2 * half)
            before = slot - 2 * half

            def step(i, carry):
                if stage == 0:
                    staged[slot + i] = held[give + i].astype(jnp.bfloat16)
                else:
                    staged[slot + i] = (
                        held[give + i]
                        + landed[before + (give - start) + i].astype(jnp.float32)
                    ).astype(jnp.bfloat16)
                return carry

            def keep_step(i, carry):
                held[keep + i] = held[keep + i] + landed[before + (keep - start) + i].astype(jnp.float32)
                return carry

            lax.fori_loop(0, half, step, 0)
            copy = pltpu.make_async_remote_copy(
                src_ref=staged.at[pl.ds(slot, half)],
                dst_ref=landed.at[pl.ds(slot, half)],
                send_sem=send_sem.at[chunk, stage],
                recv_sem=recv_sem.at[chunk, stage],
                device_id={"rep": partner(bit)},
                device_id_type=pl.DeviceIdType.MESH,
            )
            copy.start()
            copies[chunk, stage] = copy
            if stage > 0:
                lax.fori_loop(0, half, keep_step, 0)
            low[chunk].append(keep)
        elif stage < 2 * bits:
            back = 2 * bits - 1 - stage
            bit = order[back]
            size = n >> (back + 1)
            start = low[chunk][back + 1]
            if stage == bits:
                slot = chunk * n + n - 2
                result[start] = (
                    (held[start] + landed[slot].astype(jnp.float32)) * (1.0 / n)
                ).astype(jnp.bfloat16)
            copy = pltpu.make_async_remote_copy(
                src_ref=result.at[pl.ds(start, size)],
                dst_ref=result.at[pl.ds(start, size)],
                send_sem=send_sem.at[chunk, stage],
                recv_sem=recv_sem.at[chunk, stage],
                device_id={"rep": partner(bit)},
                device_id_type=pl.DeviceIdType.MESH,
            )
            copy.start()
            copies[chunk, stage] = copy
        else:
            for which, at, offset, count in pieces(chunk * n, n, split, total):
                copy = pltpu.make_async_copy(
                    result.at[pl.ds(chunk * n + offset, count)],
                    sinks[which].at[pl.ds(at, count)],
                    store_sem.at[chunk, which],
                )
                copy.start()
                stores.append(copy)

    stores = []
    waves = -(-chunks // 3)
    for tick in range(waves + 2 * bits):
        for stage in range(2 * bits, -1, -1):
            wave = tick - stage
            if 0 <= wave < waves:
                for chunk in range(3 * wave, min(3 * wave + 3, chunks)):
                    act(chunk, stage)
    for copy in copies.values():
        copy.wait_send()
    for copy in stores:
        copy.wait()


def replica_means(weight, moment):
    n = lax.axis_size("rep")
    bits = n.bit_length() - 1
    assert n == 1 << bits
    rows, columns = weight.shape
    slabs = rows // ROWS
    chunks = -(-2 * slabs // n)
    space = chunks * n
    shape = (slabs, ROWS, columns)
    out = jax.ShapeDtypeStruct(shape, jnp.bfloat16)
    sent = chunks * 2 * (n - 1) * ROWS * columns * 2
    means = pl.pallas_call(
        functools.partial(mean_kernel, n, bits, chunks),
        out_shape=(out, out),
        in_specs=[pl.BlockSpec(memory_space=pl.ANY)] * 2,
        out_specs=(pl.BlockSpec(memory_space=pl.ANY),) * 2,
        scratch_shapes=[
            pltpu.VMEM((space, ROWS, columns), jnp.float32),
            pltpu.VMEM((space, ROWS, columns), jnp.bfloat16),
            pltpu.VMEM((space, ROWS, columns), jnp.bfloat16),
            pltpu.VMEM((space, ROWS, columns), jnp.bfloat16),
            pltpu.SemaphoreType.DMA((chunks, 2)),
            pltpu.SemaphoreType.DMA((chunks, 2 * bits)),
            pltpu.SemaphoreType.DMA((chunks, 2 * bits)),
            pltpu.SemaphoreType.DMA((chunks, 2)),
        ],
        compiler_params=pltpu.CompilerParams(
            collective_id=0, has_side_effects=True, vmem_limit_bytes=62 * 1024 * 1024
        ),
        cost_estimate=pl.CostEstimate(flops=0, bytes_accessed=sent, transcendentals=0),
    )(weight.reshape(shape), moment.reshape(shape))
    return tuple(mean.reshape(rows, columns).astype(jnp.float32) for mean in means)


def gather_kernel(count, mine, everyone, send_sem, recv_sem):
    me = lax.axis_index("shard")
    barrier = pltpu.get_barrier_semaphore()
    for step in range(1, count):
        pl.semaphore_signal(barrier, inc=1, device_id={"shard": lax.rem(me + step, count)},
                            device_id_type=pl.DeviceIdType.MESH)
    pl.semaphore_wait(barrier, count - 1)
    copies = []
    for step in range(1, count):
        copy = pltpu.make_async_remote_copy(
            src_ref=mine,
            dst_ref=everyone.at[:, me],
            send_sem=send_sem.at[step - 1],
            recv_sem=recv_sem.at[step - 1],
            device_id={"shard": lax.rem(me + step, count)},
            device_id_type=pl.DeviceIdType.MESH,
        )
        copy.start()
        copies.append(copy)
    for local_step in range(mine.shape[0]):
        everyone[local_step, me] = mine[local_step]
    for copy in copies:
        copy.wait()


def gather_tokens(tokens):
    count = lax.axis_size("shard")
    steps, part, width = tokens.shape
    everyone = pl.pallas_call(
        functools.partial(gather_kernel, count),
        out_shape=jax.ShapeDtypeStruct((steps, count, part, width), tokens.dtype),
        in_specs=[pl.BlockSpec(memory_space=pltpu.VMEM)],
        out_specs=pl.BlockSpec(memory_space=pltpu.VMEM),
        scratch_shapes=[
            pltpu.SemaphoreType.DMA((count - 1,)),
            pltpu.SemaphoreType.DMA((count - 1,)),
        ],
        compiler_params=pltpu.CompilerParams(collective_id=1, has_side_effects=True),
    )(tokens)
    return everyone.reshape(steps, count * part, width)


def tile_rows(rows):
    return max(tile for tile in range(16, 401, 16) if rows % tile == 0)


def steps_kernel(params, momentum, inputs, flipped, wanted, weight, moment, half):
    rows = params.shape[0]
    tile = tile_rows(rows)
    scaling = 1.0 / float(rows) ** 0.5
    slope_scale = (2.0 / jnp.pi) ** 0.5

    def first(i, carry):
        at = pl.ds(pl.multiple_of(i * tile, tile), tile)
        half[at] = params[at].astype(jnp.bfloat16)
        return carry

    lax.fori_loop(0, rows // tile, first, 0)
    for local_step in range(inputs.shape[0]):
        pre = jnp.dot(inputs[local_step], half[...], preferred_element_type=jnp.float32) * scaling
        square = pre * pre
        bend = jnp.tanh(slope_scale * pre * (1.0 + 0.044715 * square))
        cdf = 0.5 * (1.0 + bend)
        slope = cdf + (0.5 * slope_scale) * pre * (1.0 - bend * bend) * (1.0 + 3.0 * 0.044715 * square)
        error = pre * cdf - wanted[local_step].astype(jnp.float32)
        hidden_grad = (error * slope * scaling).astype(jnp.bfloat16)
        old_weight, old_moment = (params, momentum) if local_step == 0 else (weight, moment)

        def update(i, carry):
            at = pl.ds(pl.multiple_of(i * tile, tile), tile)
            gradient = jnp.dot(flipped[local_step, at], hidden_grad, preferred_element_type=jnp.float32)
            new_moment = momentum_decay * old_moment[at] + gradient
            new_weight = old_weight[at] - learn_rate * new_moment
            moment[at] = new_moment
            weight[at] = new_weight
            if local_step + 1 < inputs.shape[0]:
                half[at] = new_weight.astype(jnp.bfloat16)
            return carry

        lax.fori_loop(0, rows // tile, update, 0)


def local_steps(params, momentum, inputs, wanted):
    rows, columns = params.shape
    steps, count, _ = inputs.shape
    block = min(256, columns)
    column = pl.BlockSpec((rows, block), lambda j: (0, j))
    out = jax.ShapeDtypeStruct((rows, columns), jnp.float32)
    return pl.pallas_call(
        steps_kernel,
        grid=(pl.cdiv(columns, block),),
        out_shape=(out, out),
        in_specs=[
            column,
            column,
            pl.BlockSpec((steps, count, rows), lambda j: (0, 0, 0)),
            pl.BlockSpec((steps, rows, count), lambda j: (0, 0, 0)),
            pl.BlockSpec((steps, count, block), lambda j: (0, 0, j)),
        ],
        out_specs=(column, column),
        scratch_shapes=[pltpu.VMEM((rows, block), jnp.bfloat16)],
        compiler_params=pltpu.CompilerParams(
            dimension_semantics=("arbitrary",), vmem_limit_bytes=60 * 1024 * 1024
        ),
    )(params, momentum, inputs, jnp.swapaxes(inputs, 1, 2), wanted)


def local(params, momentum, tokens, targets, blend_weight):
    inputs = gather_tokens(tokens[0])
    weight, moment = local_steps(params[0], momentum[0], inputs, targets[0])
    averaged, mean_moment = replica_means(weight, moment)
    blended = blend_weight * mean_moment + (1.0 - blend_weight) * moment
    return (averaged, blended[None])


def solution(mesh):
    return jax.shard_map(
        local,
        mesh=mesh,
        in_specs=(
            P("rep", None, "shard"),
            P("rep", None, "shard"),
            P("rep", None, "shard", None),
            P("rep", None, None, "shard"),
            P("shard"),
        ),
        out_specs=(P(None, "shard"), P("rep", None, "shard")),
        check_vma=False,
    )
```

```python
import functools

import jax
import jax.numpy as jnp
from jax import lax
from jax.experimental import pallas as pl
from jax.experimental.pallas import tpu as pltpu
from jax.sharding import PartitionSpec as P

learn_rate = 0.05
momentum_decay = 0.9
ROWS = 8


def bit_order(chunk, bits):
    lead = chunk % 3
    wave = chunk // 3
    rest = list(range(bits))
    if lead == 0 or bits < 3:
        return rest
    if lead == 1:
        return [1, 0] + rest[2:]
    return [2] + ([0, 1] if wave % 2 == 0 else [1, 0]) + rest[3:]


def pieces(first, count, split, total):
    out = []
    for which, (low, high) in enumerate(((0, split), (split, total))):
        begin, end = max(first, low), min(first + count, high)
        if begin < end:
            out.append((which, begin - low, begin - first, end - begin))
    return out


def mean_kernel(n, bits, chunks, weight_hbm, moment_hbm, out_w_hbm, out_m_hbm,
                held, staged, landed, result, load_sem, send_sem, recv_sem, store_sem):
    me = lax.axis_index("rep")
    sources, sinks = (weight_hbm, moment_hbm), (out_w_hbm, out_m_hbm)
    split = weight_hbm.shape[0]
    total = 2 * split
    size = n // 2

    def side(bit):
        return (me // (1 << bit)) % 2

    def partner(bit):
        return me + (1 - 2 * side(bit)) * (1 << bit)

    loads = []
    for chunk in range(chunks):
        mine = []
        for which, at, offset, count in pieces(chunk * size, size, split, total):
            mine.append(pltpu.make_async_copy(
                sources[which].at[pl.ds(at, count)],
                held.at[pl.ds(chunk * size + offset, count)],
                load_sem.at[chunk, which],
            ))
        for copy in mine:
            copy.start()
        loads.append(mine)
    padding = chunks * size - total
    if padding:
        held[pl.ds(total, padding)] = jnp.zeros((padding,) + held.shape[1:], held.dtype)

    barrier = pltpu.get_barrier_semaphore()
    for bit in range(bits):
        pl.semaphore_signal(barrier, inc=1, device_id={"rep": partner(bit)},
                            device_id_type=pl.DeviceIdType.MESH)
    pl.semaphore_wait(barrier, bits)

    copies = {}
    low = {chunk: [chunk * size] for chunk in range(chunks)}

    last = 2 * bits - 1

    def send(chunk, stage, bit, src, dst):
        copy = pltpu.make_async_remote_copy(
            src_ref=src,
            dst_ref=dst,
            send_sem=send_sem.at[chunk, stage],
            recv_sem=recv_sem.at[chunk, stage],
            device_id={"rep": partner(bit)},
            device_id_type=pl.DeviceIdType.MESH,
        )
        copy.start()
        copies[chunk, stage] = copy

    def act(chunk, stage):
        order = bit_order(chunk, bits)
        first = chunk * size
        if stage == 0:
            for copy in loads[chunk]:
                copy.wait()
        else:
            copies[chunk, stage - 1].wait_recv()
        if stage < bits:
            bit = order[stage]
            swap = stage == bits - 1
            half = 1 if swap else size >> (stage + 1)
            start = low[chunk][stage]
            keep = start if swap else start + side(bit) * half
            give = start if swap else start + (1 - side(bit)) * half
            slot = first + (size - 1 if swap else size - 2 * half)
            before = first + size - 2 * (size >> stage)

            def step(i, carry):
                value = held[give + i]
                if stage > 0:
                    value = value + landed[before + (give - start) + i].astype(jnp.float32)
                staged[slot + i] = value.astype(jnp.bfloat16)
                return carry

            def keep_step(i, carry):
                held[keep + i] = held[keep + i] + landed[before + (keep - start) + i].astype(jnp.float32)
                return carry

            lax.fori_loop(0, half, step, 0)
            send(chunk, stage, bit, staged.at[pl.ds(slot, half)], landed.at[pl.ds(slot, half)])
            if stage > 0 and not swap:
                lax.fori_loop(0, half, keep_step, 0)
            low[chunk].append(keep)
            return
        if stage == bits:
            slot = first + size - 1
            both = staged[slot].astype(jnp.float32) + landed[slot].astype(jnp.float32)
            result[low[chunk][bits - 1]] = (both * (1.0 / n)).astype(jnp.bfloat16)
        if stage < last:
            back = last - 1 - stage
            held_now = pl.ds(low[chunk][back + 1], size >> (back + 1))
            send(chunk, stage, order[back], result.at[held_now], result.at[held_now])
        else:
            for which, at, offset, count in pieces(first, size, split, total):
                copy = pltpu.make_async_copy(
                    result.at[pl.ds(first + offset, count)],
                    sinks[which].at[pl.ds(at, count)],
                    store_sem.at[chunk, which],
                )
                copy.start()
                stores.append(copy)

    stores = []
    waves = -(-chunks // 3)
    for tick in range(waves + last):
        for stage in range(last, -1, -1):
            wave = tick - stage
            if 0 <= wave < waves:
                for chunk in range(3 * wave, min(3 * wave + 3, chunks)):
                    act(chunk, stage)
    for copy in copies.values():
        copy.wait_send()
    for copy in stores:
        copy.wait()


def replica_means(weight, moment):
    n = lax.axis_size("rep")
    bits = n.bit_length() - 1
    assert n == 1 << bits
    rows, columns = weight.shape
    slabs = rows // ROWS
    chunks = -(-2 * slabs // (n // 2))
    space = chunks * (n // 2)
    shape = (slabs, ROWS, columns)
    out = jax.ShapeDtypeStruct(shape, jnp.bfloat16)
    sent = chunks * 2 * (n - 1) * ROWS * columns * 2
    means = pl.pallas_call(
        functools.partial(mean_kernel, n, bits, chunks),
        out_shape=(out, out),
        in_specs=[pl.BlockSpec(memory_space=pl.ANY)] * 2,
        out_specs=(pl.BlockSpec(memory_space=pl.ANY),) * 2,
        scratch_shapes=[
            pltpu.VMEM((space, ROWS, columns), jnp.float32),
            pltpu.VMEM((space, ROWS, columns), jnp.bfloat16),
            pltpu.VMEM((space, ROWS, columns), jnp.bfloat16),
            pltpu.VMEM((space, ROWS, columns), jnp.bfloat16),
            pltpu.SemaphoreType.DMA((chunks, 2)),
            pltpu.SemaphoreType.DMA((chunks, 2 * bits - 1)),
            pltpu.SemaphoreType.DMA((chunks, 2 * bits - 1)),
            pltpu.SemaphoreType.DMA((chunks, 2)),
        ],
        compiler_params=pltpu.CompilerParams(
            collective_id=0, has_side_effects=True, vmem_limit_bytes=62 * 1024 * 1024
        ),
        cost_estimate=pl.CostEstimate(flops=0, bytes_accessed=sent, transcendentals=0),
    )(weight.reshape(shape), moment.reshape(shape))
    return tuple(mean.reshape(rows, columns).astype(jnp.float32) for mean in means)


def gather_kernel(count, mine, everyone, send_sem, recv_sem):
    me = lax.axis_index("shard")
    barrier = pltpu.get_barrier_semaphore()
    for step in range(1, count):
        pl.semaphore_signal(barrier, inc=1, device_id={"shard": lax.rem(me + step, count)},
                            device_id_type=pl.DeviceIdType.MESH)
    pl.semaphore_wait(barrier, count - 1)
    copies = []
    for step in range(1, count):
        copy = pltpu.make_async_remote_copy(
            src_ref=mine,
            dst_ref=everyone.at[:, me],
            send_sem=send_sem.at[step - 1],
            recv_sem=recv_sem.at[step - 1],
            device_id={"shard": lax.rem(me + step, count)},
            device_id_type=pl.DeviceIdType.MESH,
        )
        copy.start()
        copies.append(copy)
    for local_step in range(mine.shape[0]):
        everyone[local_step, me] = mine[local_step]
    for copy in copies:
        copy.wait()


def gather_tokens(tokens):
    count = lax.axis_size("shard")
    steps, part, width = tokens.shape
    everyone = pl.pallas_call(
        functools.partial(gather_kernel, count),
        out_shape=jax.ShapeDtypeStruct((steps, count, part, width), tokens.dtype),
        in_specs=[pl.BlockSpec(memory_space=pltpu.VMEM)],
        out_specs=pl.BlockSpec(memory_space=pltpu.VMEM),
        scratch_shapes=[
            pltpu.SemaphoreType.DMA((count - 1,)),
            pltpu.SemaphoreType.DMA((count - 1,)),
        ],
        compiler_params=pltpu.CompilerParams(collective_id=1, has_side_effects=True),
    )(tokens)
    return everyone.reshape(steps, count * part, width)


def tile_rows(rows):
    return max(tile for tile in range(16, 401, 16) if rows % tile == 0)


def steps_kernel(params, momentum, inputs, flipped, wanted, weight, moment, half):
    rows = params.shape[0]
    tile = tile_rows(rows)
    scaling = 1.0 / float(rows) ** 0.5
    slope_scale = (2.0 / jnp.pi) ** 0.5

    def first(i, carry):
        at = pl.ds(pl.multiple_of(i * tile, tile), tile)
        half[at] = params[at].astype(jnp.bfloat16)
        return carry

    lax.fori_loop(0, rows // tile, first, 0)
    for local_step in range(inputs.shape[0]):
        pre = jnp.dot(inputs[local_step], half[...], preferred_element_type=jnp.float32) * scaling
        square = pre * pre
        bend = jnp.tanh(slope_scale * pre * (1.0 + 0.044715 * square))
        cdf = 0.5 * (1.0 + bend)
        slope = cdf + (0.5 * slope_scale) * pre * (1.0 - bend * bend) * (1.0 + 3.0 * 0.044715 * square)
        error = pre * cdf - wanted[local_step].astype(jnp.float32)
        hidden_grad = (error * slope * scaling).astype(jnp.bfloat16)
        old_weight, old_moment = (params, momentum) if local_step == 0 else (weight, moment)

        def update(i, carry):
            at = pl.ds(pl.multiple_of(i * tile, tile), tile)
            gradient = jnp.dot(flipped[local_step, at], hidden_grad, preferred_element_type=jnp.float32)
            new_moment = momentum_decay * old_moment[at] + gradient
            new_weight = old_weight[at] - learn_rate * new_moment
            moment[at] = new_moment
            weight[at] = new_weight
            if local_step + 1 < inputs.shape[0]:
                half[at] = new_weight.astype(jnp.bfloat16)
            return carry

        lax.fori_loop(0, rows // tile, update, 0)


def local_steps(params, momentum, inputs, wanted):
    rows, columns = params.shape
    steps, count, _ = inputs.shape
    block = min(256, columns)
    column = pl.BlockSpec((rows, block), lambda j: (0, j))
    out = jax.ShapeDtypeStruct((rows, columns), jnp.float32)
    return pl.pallas_call(
        steps_kernel,
        grid=(pl.cdiv(columns, block),),
        out_shape=(out, out),
        in_specs=[
            column,
            column,
            pl.BlockSpec((steps, count, rows), lambda j: (0, 0, 0)),
            pl.BlockSpec((steps, rows, count), lambda j: (0, 0, 0)),
            pl.BlockSpec((steps, count, block), lambda j: (0, 0, j)),
        ],
        out_specs=(column, column),
        scratch_shapes=[pltpu.VMEM((rows, block), jnp.bfloat16)],
        compiler_params=pltpu.CompilerParams(
            dimension_semantics=("arbitrary",), vmem_limit_bytes=60 * 1024 * 1024
        ),
    )(params, momentum, inputs, jnp.swapaxes(inputs, 1, 2), wanted)


def local(params, momentum, tokens, targets, blend_weight):
    inputs = gather_tokens(tokens[0])
    weight, moment = local_steps(params[0], momentum[0], inputs, targets[0])
    averaged, mean_moment = replica_means(weight, moment)
    blended = blend_weight * mean_moment + (1.0 - blend_weight) * moment
    return (averaged, blended[None])


def solution(mesh):
    return jax.shard_map(
        local,
        mesh=mesh,
        in_specs=(
            P("rep", None, "shard"),
            P("rep", None, "shard"),
            P("rep", None, "shard", None),
            P("rep", None, None, "shard"),
            P("shard"),
        ),
        out_specs=(P(None, "shard"), P("rep", None, "shard")),
        check_vma=False,
    )
```
